32 devices in a mesh: ep: 4 (over x, core), fsdp: 8 (over z, y).
Axes of the slice: x: 2, y: 2, z: 4, core: 2. Of those that a mesh axis runs over, the one named last changes fastest.
Arguments:
- train_gate: float32 [128, 2048, 768], P('ep', 'fsdp'), may hold values from -0.1875 to 0.1875
- other_gate: bfloat16 [128, 2048, 768], P('ep', 'fsdp'), may hold values from -0.0625 to 0.0625
- train_up: float32 [128, 2048, 768], P('ep', 'fsdp'), may hold values from -0.1875 to 0.1875
- other_up: bfloat16 [128, 2048, 768], P('ep', 'fsdp'), may hold values from -0.0625 to 0.0625
- router_weight: float32 [2048, 128], P('fsdp', 'ep'), may hold values from -0.125 to 0.125
- router_gain: float32 [2048], P('fsdp'), may hold values from 0.25 to 1.75
Outputs:
- ready_gate: bfloat16 [128, 2048, 768], P('ep', None, 'fsdp')
- ready_up: bfloat16 [128, 2048, 768], P('ep', None, 'fsdp')
- scale_gate: float32 [128, 768], P('ep', 'fsdp')
- scale_up: float32 [128, 768], P('ep', 'fsdp')
- serve_router: bfloat16 [2048, 128], replicated
The draws below stay inside these ranges and needn't reach their ends.
All inputs are finite; a program needn't handle non-finite values. Where the reference program divides by a largest or mean magnitude, that divisor is 1e-20 or more.
Results may differ from the reference program's by a relative error of at most 0.001.
Values may be sent and summed in bfloat16 or wider, within the bound.
A program may use at most 256 MiB of HBM per device.

```python
import jax
import jax.numpy as jnp

EXPERTS = 128
D_MODEL = 2048
D_EXPERT = 768


def spiked(values, stream_key, source, target, parts, factor):
    def block_of(axis_at):
        return (jnp.arange(values.shape[axis_at]) // (values.shape[axis_at] // parts)).reshape((-1,) + (1,) * (values.ndim - 1 - axis_at))

    first = jax.random.permutation(stream_key, parts)[block_of(target)]
    second = (block_of(target) + parts // 2) % parts
    return jnp.where((block_of(source) == first) | (block_of(source) == second), factor * values, values)


def level_of(own_key, shape, split, least, top_value):
    def one(position, parts):
        draws = jax.random.uniform(jax.random.fold_in(jax.random.fold_in(own_key, 6), position), (parts,), jnp.float32, least / len(split), top_value / len(split))
        return jnp.repeat(jnp.exp(draws), shape[position] // parts).reshape((-1,) + (1,) * (len(shape) - position - 1))

    gain = one(*split[0])
    for cut in split[1:]:
        gain = gain * one(*cut)
    return gain


def normal_values(key, extent, deviation, bound, cuts=(), held_as=jnp.bfloat16):
    level = level_of(key, extent, cuts, -0.22, 0.18) if cuts else 1.0
    values = jax.random.normal(key, extent, jnp.float32) * deviation * level
    return jnp.minimum(jnp.maximum(values, -bound), bound).astype(held_as)


def noise_with(stream_key, shape, spread, reach, cuts, heavy, held_as=jnp.bfloat16):
    entries = spread * jax.random.normal(stream_key, shape, jnp.float32)
    if cuts:
        entries = entries * level_of(stream_key, shape, cuts, -0.22, 0.18)
    return jnp.clip(spiked(entries, jax.random.fold_in(stream_key, 3), *heavy), -reach, reach).astype(held_as)


def setup_inputs(seed: int = 0) -> dict:
    key_of = jax.random.split(jax.random.key(seed), 7)
    return {
        "train_gate": noise_with(key_of[0], (EXPERTS, D_MODEL, D_EXPERT), D_MODEL ** -0.5, 0.1875, ((0, 4), (1, 8)), (1, 2, 8, 2.0), jnp.float32),
        "other_gate": normal_values(key_of[1], (EXPERTS, D_MODEL, D_EXPERT), (D_MODEL * 4) ** -0.5, 0.0625, ((0, 4), (1, 8))),
        "train_up": noise_with(key_of[2], (EXPERTS, D_MODEL, D_EXPERT), D_MODEL ** -0.5, 0.1875, ((0, 4), (1, 8)), (1, 2, 8, 2.0), jnp.float32),
        "other_up": normal_values(key_of[3], (EXPERTS, D_MODEL, D_EXPERT), (D_MODEL * 4) ** -0.5, 0.0625, ((0, 4), (1, 8))),
        "router_weight": normal_values(key_of[4], (D_MODEL, EXPERTS), D_MODEL ** -0.5, 0.125, ((0, 8), (1, 4)), jnp.float32),
        "router_gain": jnp.clip(1.0 + 0.15 * jax.random.normal(key_of[5], (D_MODEL,), jnp.float32), 0.25, 1.75),
    }


def reference(train_gate, other_gate, train_up, other_up, router_weight, router_gain):
    latest_gate = train_gate + other_gate.astype(jnp.float32)
    latest_up = train_up + other_up.astype(jnp.float32)
    scale_gate = jnp.sum(jnp.abs(latest_gate), axis=1) / D_MODEL
    ready_gate = (latest_gate / jnp.expand_dims(scale_gate, 1)).astype(jnp.bfloat16)
    scale_up = jnp.sum(jnp.abs(latest_up), axis=1) / D_MODEL
    ready_up = (latest_up / jnp.expand_dims(scale_up, 1)).astype(jnp.bfloat16)
    serve_router = (router_weight * router_gain[:, None]).astype(jnp.bfloat16)
    return ready_gate, ready_up, scale_gate, scale_up, serve_router
```

```python
import functools

import jax
import jax.numpy as jnp
from jax import lax
from jax.experimental import pallas as pl
from jax.experimental.pallas import tpu as pltpu
from jax.sharding import PartitionSpec as P

MESH = pl.DeviceIdType.MESH
SLOTS = 3
RING = 8
LAG = 4
f32, bf16 = jnp.float32, jnp.bfloat16


def plain_device(train_gate, other_gate, train_up, other_up, router_weight, router_gain):
    latest_gate = train_gate + other_gate.astype(jnp.float32)
    latest_up = train_up + other_up.astype(jnp.float32)
    depth = train_gate.shape[1] * lax.axis_size("fsdp")
    total_gate, total_up = lax.psum(
        (jnp.sum(jnp.abs(latest_gate), axis=1), jnp.sum(jnp.abs(latest_up), axis=1)), "fsdp"
    )
    scale_gate = total_gate / depth
    scale_up = total_up / depth
    narrow_gate = (latest_gate / jnp.expand_dims(scale_gate, 1)).astype(jnp.bfloat16)
    narrow_up = (latest_up / jnp.expand_dims(scale_up, 1)).astype(jnp.bfloat16)
    ready_gate = lax.all_to_all(narrow_gate, "fsdp", split_axis=2, concat_axis=1, tiled=True)
    ready_up = lax.all_to_all(narrow_up, "fsdp", split_axis=2, concat_axis=1, tiled=True)
    width = ready_gate.shape[2]
    start = lax.axis_index("fsdp") * width
    scale_gate = lax.dynamic_slice_in_dim(scale_gate, start, width, axis=1)
    scale_up = lax.dynamic_slice_in_dim(scale_up, start, width, axis=1)
    part_router = (router_weight * router_gain[:, None]).astype(jnp.bfloat16)
    row_router = lax.all_gather(part_router, "fsdp", axis=0, tiled=True)
    serve_router = lax.all_gather(row_router, "ep", axis=1, tiled=True)
    return (ready_gate, ready_up, scale_gate, scale_up, serve_router)


def far_first(n):
    return sorted(range(1, n), key=lambda d: (abs(d - n // 2), d))


def drain(ref, sem):
    pltpu.make_async_copy(ref, ref, sem).wait()


class Stream:
    def __init__(self, sources, wide, narrow, sem):
        self.sources, self.wide, self.narrow, self.sem = sources, wide, narrow, sem

    def loads(self, e):
        slot = lax.rem(e, SLOTS)
        return [
            pltpu.make_async_copy(src.at[e], dst.at[m, slot], self.sem.at[k, m, slot])
            for m, pair in enumerate(self.sources)
            for k, (src, dst) in enumerate(zip(pair, (self.wide, self.narrow)))
        ]

    def prime(self, low, last):
        for i in range(SLOTS - 1):
            @pl.when(low + i < last)
            def _():
                for copy in self.loads(low + i):
                    copy.start()

    def one(self, e, last, body):
        @pl.when(e + SLOTS - 1 < last)
        def _():
            for copy in self.loads(e + SLOTS - 1):
                copy.start()

        copies = self.loads(e)
        slot = lax.rem(e, SLOTS)
        for m in range(2):
            copies[2 * m].wait()
            copies[2 * m + 1].wait()
            body(e, m, self.wide.at[m, slot], self.narrow.at[m, slot])

    def run(self, low, high, last, body):
        def step(i, _):
            self.one(low + i, last, body)
            return 0

        lax.fori_loop(0, high - low, step, 0)


def row_sums(wide, narrow, out, at):
    depth, width = wide.shape
    block = 256 if width % 256 == 0 else 128
    for c in range(0, width, block):
        total = jnp.zeros((16, block), f32)
        for r in range(0, depth, 16):
            total += jnp.abs(wide[r:r + 16, c:c + block] + narrow[r:r + 16, c:c + block].astype(f32))
        out[at, c:c + block] = jnp.sum(total, axis=0, keepdims=True)


def sender(n, me, peers, send, scales, readys, base, own_sem, send_sem, recv_sem):
    def body(e, m, wide, narrow):
        depth, width = wide.shape
        piece = width // n
        inverse = 1.0 / scales[m][pl.ds(e, 1), :]
        at = e - base
        for c in range(0, width, 128):
            latest = wide[:, c:c + 128] + narrow[:, c:c + 128].astype(f32)
            value = latest * inverse[:, c:c + 128]
            send[m, at, c:c + 128, :] = value.T.astype(bf16)
        place = readys[m].at[at, :, pl.ds(pl.multiple_of(me * depth, 128), depth)]
        for peer in peers:
            pltpu.make_async_remote_copy(
                src_ref=send.at[m, at, pl.ds(pl.multiple_of(peer * piece, 16), piece), :],
                dst_ref=place,
                send_sem=send_sem.at[m],
                recv_sem=recv_sem.at[m],
                device_id={"fsdp": peer},
                device_id_type=MESH,
            ).start()
        own = send.at[m, at, pl.ds(pl.multiple_of(me * piece, 16), piece), :]
        if own_sem is None:
            place[...] = own[...]
        else:
            pltpu.make_async_copy(own, place, own_sem.at[m]).start()

    return body


def finish(n, count, send, readys, own_sem, send_sem, recv_sem):
    width, depth = send.shape[2:]
    piece = width // n
    for m in range(2):
        some = pl.ds(0, count)
        if own_sem is not None:
            drain(send.at[m, some, pl.ds(0, piece), :], own_sem.at[m])
        drain(send.at[m, some, pl.ds(0, width - piece), :], send_sem.at[m])
        drain(readys[m].at[some, :, pl.ds(0, (n - 1) * depth)], recv_sem.at[m])


def bulk_kernel(n, p, cut, more, tg, og, tu, ou, rw, rgain, ready_gate, ready_up, scale_gate, scale_up, router,
                wide_s, narrow_s, wide_r, narrow_r, send, land_0, part_a, land_a, tot_a,
                part_z, land_z, sum_z, far_z, tot_z, rows_r, all_r,
                in_s, in_r, own_sem, send_sem, recv_sem, small_send, small_recv, r_send, r_recv):
    experts, depth, width = tg.shape
    half = n // 2
    me = lax.axis_index("fsdp")
    group = lax.axis_index("ep")
    odd = lax.rem(group, 2) == 1
    stop = jnp.where(odd, cut + more, cut)
    mine = lax.rem(me, half)
    side = me - mine
    first, second = 1, 1 + half
    readys, scales = (ready_gate, ready_up), (scale_gate, scale_up)
    peers = [(me + d) % n for d in far_first(n)]
    near = [side + lax.rem(mine + d, half) for d in range(1, half)]
    near_at = [lax.rem(mine + d, half) for d in range(1, half)]
    far = (me + half) % n
    twins = [(group + d) % p for d in range(1, p)]
    sources = ((tg, og), (tu, ou))
    sums = Stream(sources, wide_s, narrow_s, in_s)
    ready = Stream(sources, wide_r, narrow_r, in_r)

    barrier = pltpu.get_barrier_semaphore()
    sums.prime(0, experts)
    for peer in peers:
        pl.semaphore_signal(barrier, inc=1, device_id={"fsdp": peer}, device_id_type=MESH)
    for twin in twins:
        pl.semaphore_signal(barrier, inc=1, device_id={"ep": twin}, device_id_type=MESH)

    def push(src, dst, axis, target, s, r):
        pltpu.make_async_remote_copy(
            src_ref=src, dst_ref=dst, send_sem=s, recv_sem=r,
            device_id={axis: target}, device_id_type=MESH,
        ).start()

    def sums_0(e, m, wide, narrow):
        row_sums(wide, narrow, land_0.at[me], pl.ds(m, 1))

    def sums_a(e, m, wide, narrow):
        row_sums(wide, narrow, part_a.at[(e - first) * 2 + m], pl.ds(0, 1))

    share = part_z.shape[1]

    def sums_z(e, m, wide, narrow):
        at = (e - second) * 2 + m
        row_sums(wide, narrow, part_z.at[at // share], pl.ds(at % share, 1))

    def keep(e, m, total):
        scales[m][pl.ds(e, 1), :] = total / (n * depth)

    begin_0 = sender(n, me, peers, send, scales, readys, 0, own_sem.at[0], send_sem.at[0], recv_sem.at[0])
    begin_1 = sender(n, me, peers, send, scales, readys, 0, own_sem.at[1], send_sem.at[1], recv_sem.at[1])

    sums.one(0, experts, sums_0)
    pl.semaphore_wait(barrier, n - 1 + p - 1)
    for peer in peers:
        push(land_0.at[me], land_0.at[me], "fsdp", peer, small_send.at[0], small_recv.at[0])
    ready.prime(0, stop)
    sums.run(first, second, experts, sums_a)
    for peer in peers:
        push(part_a.at[peer], land_a.at[me], "fsdp", peer, small_send.at[1], small_recv.at[1])
    land_a[me] = part_a[me]
    drain(land_0.at[pl.ds(0, n - 1)], small_recv.at[0])
    total_0 = jnp.sum(land_0[...], axis=0)
    for m in range(2):
        keep(0, m, total_0[m:m + 1])
    ready.one(0, stop, begin_0)
    drain(land_a.at[pl.ds(0, n - 1)], small_recv.at[1])
    tot_a[me] = jnp.sum(land_a[...], axis=0)
    for peer in peers:
        push(tot_a.at[me], tot_a.at[me], "fsdp", peer, small_send.at[2], small_recv.at[2])
    rows_r[me] = (rw[...] * rgain[...]).astype(bf16)
    push(rows_r.at[me], rows_r.at[me], "fsdp", far, r_send.at[0], r_recv.at[0])
    some = second + (experts - second) * 2 // 5
    sums.run(second, some, experts, sums_z)
    drain(tot_a.at[pl.ds(0, n - 1)], small_recv.at[2])
    for k in range(n):
        keep(first + k // 2, k % 2, tot_a[k])
    ready.run(1, 2, stop, begin_0)
    sums.run(some, experts, experts, sums_z)
    spare = half * share - 2 * (experts - second)
    if spare:
        part_z[half - 1, share - spare:, :] = jnp.zeros((spare, width), f32)
    for peer, at in zip(near, near_at):
        push(part_z.at[at], land_z.at[mine], "fsdp", peer, small_send.at[3], small_recv.at[3])
    land_z[mine] = part_z[mine]
    ready.run(2, 3, stop, begin_0)
    drain(land_z.at[pl.ds(0, half - 1)], small_recv.at[3])
    sum_z[...] = jnp.sum(land_z[...], axis=0)
    push(sum_z, far_z, "fsdp", far, small_send.at[4], small_recv.at[4])
    drain(rows_r.at[0], r_recv.at[0])
    for peer in near:
        push(rows_r.at[me], rows_r.at[me], "fsdp", peer, r_send.at[1], r_recv.at[1])
        push(rows_r.at[far], rows_r.at[far], "fsdp", peer, r_send.at[1], r_recv.at[1])
    ready.run(3, 4, stop, begin_0)
    drain(far_z, small_recv.at[4])
    tot_z[mine] = sum_z[...] + far_z[...]
    for peer in near:
        push(tot_z.at[mine], tot_z.at[mine], "fsdp", peer, small_send.at[5], small_recv.at[5])
    ready.run(4, second, stop, begin_0)
    drain(tot_z.at[pl.ds(0, half - 1)], small_recv.at[5])

    def keep_z(i, _):
        for m in range(2):
            at = i * 2 + m
            keep(second + i, m, tot_z[at // share, pl.ds(at % share, 1), :])
        return 0

    lax.fori_loop(0, experts - second, keep_z, 0)
    ready.run(second, cut, stop, begin_0)
    ready.run(cut, stop, stop, begin_1)
    drain(rows_r.at[pl.ds(0, n - 2)], r_recv.at[1])
    for twin in twins:
        push(rows_r, all_r.at[group], "ep", twin, r_send.at[2], r_recv.at[2])
    all_r[group] = rows_r[...]
    if p > 1:
        drain(all_r.at[pl.ds(0, p - 1)], r_recv.at[2])
    for f in range(n):
        block = all_r[:, f].astype(f32)
        block = block.reshape(block.shape[0] * block.shape[1], depth)
        router[f * depth:(f + 1) * depth, :] = block.T.astype(bf16)
    drain(land_0.at[pl.ds(0, n - 1)], small_send.at[0])
    drain(part_a.at[pl.ds(0, n - 1)], small_send.at[1])
    drain(tot_a.at[pl.ds(0, n - 1)], small_send.at[2])
    drain(part_z.at[pl.ds(0, half - 1)], small_send.at[3])
    drain(sum_z, small_send.at[4])
    drain(tot_z.at[pl.ds(0, half - 1)], small_send.at[5])
    drain(rows_r.at[0], r_send.at[0])
    drain(rows_r.at[pl.ds(0, n - 2)], r_send.at[1])
    if p > 1:
        drain(all_r.at[pl.ds(0, p - 1)], r_send.at[2])
    finish(n, cut, send, readys, own_sem.at[0], send_sem.at[0], recv_sem.at[0])

    @pl.when(odd)
    def _():
        finish(n, more, send, readys, own_sem.at[1], send_sem.at[1], recv_sem.at[1])


def rest_kernel(n, cut, more, tg, og, tu, ou, scale_gate, scale_up, ready_gate, ready_up,
                wide, narrow, send, in_sem, send_sem, recv_sem):
    experts = tg.shape[0]
    me = lax.axis_index("fsdp")
    odd = lax.rem(lax.axis_index("ep"), 2) == 1
    start = jnp.where(odd, cut + more, cut)
    readys, scales = (ready_gate, ready_up), (scale_gate, scale_up)
    peers = [(me + d) % n for d in far_first(n)]
    ready = Stream(((tg, og), (tu, ou)), wide, narrow, in_sem)
    barrier = pltpu.get_barrier_semaphore()
    for peer in peers:
        pl.semaphore_signal(barrier, inc=1, device_id={"fsdp": peer}, device_id_type=MESH)
    ready.prime(start, experts)
    pl.semaphore_wait(barrier, n - 1)
    begin = [
        sender(n, me, peers, send, scales, readys, cut, None, send_sem.at[k], recv_sem.at[k])
        for k in range(2)
    ]
    ready.run(start, cut + more, experts, begin[1])
    ready.run(cut + more, experts, experts, begin[0])
    finish(n, experts - cut - more, send, readys, None, send_sem.at[0], recv_sem.at[0])

    @pl.when(jnp.logical_not(odd))
    def _():
        finish(n, more, send, readys, None, send_sem.at[1], recv_sem.at[1])


def copy_through(pairs, count, buffer, in_sem, out_sem):
    def bring(i, k):
        slot = lax.rem(i, RING)
        return pltpu.make_async_copy(pairs[k][0].at[i], buffer.at[k, slot], in_sem.at[k, slot])

    def give(i, k):
        slot = lax.rem(i, RING)
        return pltpu.make_async_copy(buffer.at[k, slot], pairs[k][1].at[i], out_sem.at[k, slot])

    def opening(i, _):
        for k in range(2):
            bring(i, k).start()
        return 0

    lax.fori_loop(0, jnp.minimum(count, RING), opening, 0)

    def step(i, _):
        @pl.when(i < count)
        def _():
            for k in range(2):
                bring(i, k).wait()
                give(i, k).start()

        @pl.when(i >= LAG)
        def _():
            for k in range(2):
                give(i - LAG, k).wait()

            @pl.when(i - LAG + RING < count)
            def _():
                for k in range(2):
                    bring(i - LAG + RING, k).start()

        return 0

    lax.fori_loop(0, count + LAG, step, 0)


def own_columns(n, scale, out):
    me = lax.axis_index("fsdp")
    piece = out.shape[1]
    value = jnp.zeros(out.shape, out.dtype)
    for j in range(n):
        value = jnp.where(me == j, scale[:, j * piece:(j + 1) * piece], value)
    out[...] = value


def place_kernel(n, cut, more, got_gate, got_up, scale_gate, scale_up, router,
                 gate, up, own_gate, own_up, full_gate, full_up, router_out, buffer, in_sem, out_sem):
    odd = lax.rem(lax.axis_index("ep"), 2) == 1
    high = jnp.where(odd, cut + more, cut)
    copy_through(((got_gate, gate), (got_up, up)), high, buffer, in_sem, out_sem)
    own_columns(n, scale_gate, own_gate)
    own_columns(n, scale_up, own_up)
    full_gate[...] = scale_gate[...]
    full_up[...] = scale_up[...]
    router_out[...] = router[...]


def end_kernel(n, cut, more, got_gate, got_up, had_gate, had_up, gate, up, sem):
    odd = lax.rem(lax.axis_index("ep"), 2) == 1
    experts = gate.shape[0]
    early, late = pl.ds(0, more), pl.ds(more, experts - cut - more)

    def copies(some, low, count, k):
        return [
            pltpu.make_async_copy(got.at[some], out.at[pl.ds(low, count)], sem.at[k, m])
            for m, (got, out) in enumerate(((got_gate, gate), (got_up, up)))
        ]

    both = copies(late, cut + more, experts - cut - more, 0)
    for copy in both:
        copy.start()

    @pl.when(jnp.logical_not(odd))
    def _():
        others = copies(early, cut, more, 1)
        for copy in others:
            copy.start()
        for copy in others:
            copy.wait()

    for copy in both:
        copy.wait()


def sending_device(n, p, train_gate, other_gate, train_up, other_up, router_weight, router_gain):
    experts, depth, width = train_gate.shape
    piece = width // n
    columns = router_weight.shape[1]
    half = n // 2
    share = -(-2 * (experts - 1 - half) // half)
    tail = experts // 16
    more = experts // 8
    cut = experts - tail - more
    bulk, rest = cut + more, experts - cut
    anywhere = pl.BlockSpec(memory_space=pltpu.HBM)
    vmem = pl.BlockSpec(memory_space=pltpu.VMEM)
    shape = jax.ShapeDtypeStruct
    full = shape((experts, width), f32)
    own = shape((experts, piece), f32)
    whole = shape((experts, piece, n * depth), bf16)
    routed = shape((n * depth, p * columns), bf16)
    dma = pltpu.SemaphoreType.DMA
    got_gate, got_up, scale_gate, scale_up, router = pl.pallas_call(
        functools.partial(bulk_kernel, n, p, cut, more),
        out_shape=(shape((bulk, piece, n * depth), bf16),) * 2 + (full, full, routed),
        in_specs=[anywhere] * 4 + [vmem] * 2,
        out_specs=(anywhere, anywhere, vmem, vmem, vmem),
        scratch_shapes=[
            pltpu.VMEM((2, SLOTS, depth, width), f32),
            pltpu.VMEM((2, SLOTS, depth, width), bf16),
            pltpu.VMEM((2, SLOTS, depth, width), f32),
            pltpu.VMEM((2, SLOTS, depth, width), bf16),
            pltpu.VMEM((2, bulk, width, depth), bf16),
            pltpu.VMEM((n, 2, width), f32),
            *[pltpu.VMEM((n, 1, width), f32)] * 3,
            *[pltpu.VMEM((half, share, width), f32)] * 2,
            *[pltpu.VMEM((share, width), f32)] * 2,
            pltpu.VMEM((half, share, width), f32),
            pltpu.VMEM((n, columns, depth), bf16),
            pltpu.VMEM((p, n, columns, depth), bf16),
            dma((2, 2, SLOTS)), dma((2, 2, SLOTS)), dma((2, 2)), dma((2, 2)), dma((2, 2)),
            dma((6,)), dma((6,)), dma((3,)), dma((3,)),
        ],
        compiler_params=pltpu.CompilerParams(
            collective_id=0, has_side_effects=True, vmem_limit_bytes=60 * 2**20
        ),
        name="send_bulk",
    )(train_gate, other_gate, train_up, other_up, router_weight.T, router_gain[None, :])
    ring = [pltpu.VMEM((2, RING, piece, n * depth), bf16), dma((2, RING)), dma((2, RING))]
    gate, up, own_gate, own_up, scale_gate, scale_up, router = pl.pallas_call(
        functools.partial(place_kernel, n, cut, more),
        out_shape=(whole, whole, own, own, full, full, routed),
        in_specs=[anywhere] * 2 + [vmem] * 3,
        out_specs=(anywhere, anywhere, vmem, vmem, vmem, vmem, vmem),
        scratch_shapes=ring,
        compiler_params=pltpu.CompilerParams(vmem_limit_bytes=40 * 2**20),
        name="place_bulk",
    )(got_gate, got_up, scale_gate, scale_up, router)
    got_gate, got_up = pl.pallas_call(
        functools.partial(rest_kernel, n, cut, more),
        out_shape=(shape((rest, piece, n * depth), bf16),) * 2,
        in_specs=[anywhere] * 4 + [vmem] * 2,
        out_specs=(vmem, vmem),
        scratch_shapes=[
            pltpu.VMEM((2, SLOTS, depth, width), f32),
            pltpu.VMEM((2, SLOTS, depth, width), bf16),
            pltpu.VMEM((2, rest, width, depth), bf16),
            dma((2, 2, SLOTS)), dma((2, 2)), dma((2, 2)),
        ],
        compiler_params=pltpu.CompilerParams(
            collective_id=1, has_side_effects=True, vmem_limit_bytes=40 * 2**20
        ),
        name="send_rest",
    )(train_gate, other_gate, train_up, other_up, scale_gate, scale_up)
    gate, up = pl.pallas_call(
        functools.partial(end_kernel, n, cut, more),
        out_shape=(whole, whole),
        in_specs=[vmem] * 2 + [anywhere] * 2,
        out_specs=(anywhere, anywhere),
        scratch_shapes=[dma((2, 2))],
        input_output_aliases={2: 0, 3: 1},
        compiler_params=pltpu.CompilerParams(vmem_limit_bytes=40 * 2**20),
        name="place_rest",
    )(got_gate, got_up, gate, up)
    return (jnp.swapaxes(gate, 1, 2), jnp.swapaxes(up, 1, 2), own_gate, own_up, router)


def solution(mesh):
    n, p = mesh.shape["fsdp"], mesh.shape["ep"]

    def per_device(*args):
        experts, depth, width = args[0].shape
        fits = (
            depth % 128 == 0 and width % (16 * n) == 0 and width % 128 == 0 and n % 4 == 0
            and experts % 16 == 0 and experts >= n + 8 and args[4].shape[1] % 16 == 0
            and 2 * experts * depth * width * 2 <= 2**25
        )
        return sending_device(n, p, *args) if fits else plain_device(*args)

    matrix = P("ep", "fsdp", None)
    in_specs = (matrix, matrix, matrix, matrix, P("fsdp", "ep"), P("fsdp"))
    out_specs = (P("ep", None, "fsdp"), P("ep", None, "fsdp"), P("ep", "fsdp"), P("ep", "fsdp"), P())
    return jax.shard_map(
        per_device, mesh=mesh, in_specs=in_specs, out_specs=out_specs, check_vma=False
    )
```

```python
import functools

import jax
import jax.numpy as jnp
from jax import lax
from jax.experimental import pallas as pl
from jax.experimental.pallas import tpu as pltpu
from jax.sharding import PartitionSpec as P

MESH = pl.DeviceIdType.MESH
SLOTS = 3
RING = 20
SLOW = 2
f32, bf16 = jnp.float32, jnp.bfloat16


def plain_device(train_gate, other_gate, train_up, other_up, router_weight, router_gain):
    latest_gate = train_gate + other_gate.astype(jnp.float32)
    latest_up = train_up + other_up.astype(jnp.float32)
    depth = train_gate.shape[1] * lax.axis_size("fsdp")
    total_gate, total_up = lax.psum(
        (jnp.sum(jnp.abs(latest_gate), axis=1), jnp.sum(jnp.abs(latest_up), axis=1)), "fsdp"
    )
    scale_gate = total_gate / depth
    scale_up = total_up / depth
    narrow_gate = (latest_gate / jnp.expand_dims(scale_gate, 1)).astype(jnp.bfloat16)
    narrow_up = (latest_up / jnp.expand_dims(scale_up, 1)).astype(jnp.bfloat16)
    ready_gate = lax.all_to_all(narrow_gate, "fsdp", split_axis=2, concat_axis=1, tiled=True)
    ready_up = lax.all_to_all(narrow_up, "fsdp", split_axis=2, concat_axis=1, tiled=True)
    width = ready_gate.shape[2]
    start = lax.axis_index("fsdp") * width
    scale_gate = lax.dynamic_slice_in_dim(scale_gate, start, width, axis=1)
    scale_up = lax.dynamic_slice_in_dim(scale_up, start, width, axis=1)
    part_router = (router_weight * router_gain[:, None]).astype(jnp.bfloat16)
    row_router = lax.all_gather(part_router, "fsdp", axis=0, tiled=True)
    serve_router = lax.all_gather(row_router, "ep", axis=1, tiled=True)
    return (ready_gate, ready_up, scale_gate, scale_up, serve_router)


def far_first(n):
    return sorted(range(1, n), key=lambda d: (abs(d - n // 2), d))


def drain(ref, sem):
    pltpu.make_async_copy(ref, ref, sem).wait()


class Stream:
    def __init__(self, sources, wide, narrow, sem):
        self.sources, self.wide, self.narrow, self.sem = sources, wide, narrow, sem

    def loads(self, e):
        slot = lax.rem(e, SLOTS)
        return [
            pltpu.make_async_copy(src.at[e], dst.at[m, slot], self.sem.at[k, m, slot])
            for m, pair in enumerate(self.sources)
            for k, (src, dst) in enumerate(zip(pair, (self.wide, self.narrow)))
        ]

    def prime(self, low, last):
        for i in range(SLOTS - 1):
            @pl.when(low + i < last)
            def _():
                for copy in self.loads(low + i):
                    copy.start()

    def one(self, e, last, body):
        @pl.when(e + SLOTS - 1 < last)
        def _():
            for copy in self.loads(e + SLOTS - 1):
                copy.start()

        copies = self.loads(e)
        slot = lax.rem(e, SLOTS)
        for m in range(2):
            copies[2 * m].wait()
            copies[2 * m + 1].wait()
            body(e, m, self.wide.at[m, slot], self.narrow.at[m, slot])

    def run(self, low, high, last, body):
        def step(i, _):
            self.one(low + i, last, body)
            return 0

        lax.fori_loop(0, high - low, step, 0)


def row_sums(wide, narrow, out, at):
    depth, width = wide.shape
    block = 256 if width % 256 == 0 else 128
    for c in range(0, width, block):
        total = jnp.zeros((16, block), f32)
        for r in range(0, depth, 16):
            total += jnp.abs(wide[r:r + 16, c:c + block] + narrow[r:r + 16, c:c + block].astype(f32))
        out[at, c:c + block] = jnp.sum(total, axis=0, keepdims=True)


def sender(n, me, peers, send, scales, readys, base, own_sem, send_sem, recv_sem):
    def body(e, m, wide, narrow):
        depth, width = wide.shape
        piece = width // n
        inverse = 1.0 / scales[m][pl.ds(e, 1), :]
        at = e - base
        for c in range(0, width, 128):
            latest = wide[:, c:c + 128] + narrow[:, c:c + 128].astype(f32)
            value = latest * inverse[:, c:c + 128]
            send[m, at, c:c + 128, :] = value.T.astype(bf16)
        place = readys[m].at[at, :, pl.ds(pl.multiple_of(me * depth, 128), depth)]
        for peer in peers:
            pltpu.make_async_remote_copy(
                src_ref=send.at[m, at, pl.ds(pl.multiple_of(peer * piece, 16), piece), :],
                dst_ref=place,
                send_sem=send_sem.at[m],
                recv_sem=recv_sem.at[m],
                device_id={"fsdp": peer},
                device_id_type=MESH,
            ).start()
        own = send.at[m, at, pl.ds(pl.multiple_of(me * piece, 16), piece), :]
        if own_sem is None:
            place[...] = own[...]
        else:
            pltpu.make_async_copy(own, place, own_sem.at[m]).start()

    return body


def finish(n, count, send, readys, own_sem, send_sem, recv_sem):
    width, depth = send.shape[2:]
    piece = width // n
    for m in range(2):
        some = pl.ds(0, count)
        if own_sem is not None:
            drain(send.at[m, some, pl.ds(0, piece), :], own_sem.at[m])
        drain(send.at[m, some, pl.ds(0, width - piece), :], send_sem.at[m])
        drain(readys[m].at[some, :, pl.ds(0, (n - 1) * depth)], recv_sem.at[m])


def bulk_kernel(n, p, cut, more, tg, og, tu, ou, rw, rgain, ready_gate, ready_up, scale_gate, scale_up, router,
                wide_s, narrow_s, wide_r, narrow_r, send, land_0, part_a, land_a, tot_a,
                part_z, land_z, sum_z, far_z, tot_z, rows_r, all_r,
                in_s, in_r, own_sem, send_sem, recv_sem, small_send, small_recv, r_send, r_recv):
    experts, depth, width = tg.shape
    half = n // 2
    me = lax.axis_index("fsdp")
    group = lax.axis_index("ep")
    odd = lax.rem(group, 2) == 1
    stop = jnp.where(odd, cut + more, cut)
    mine = lax.rem(me, half)
    side = me - mine
    first, second = 1, 1 + half
    readys, scales = (ready_gate, ready_up), (scale_gate, scale_up)
    peers = [(me + d) % n for d in far_first(n)]
    near = [side + lax.rem(mine + d, half) for d in range(1, half)]
    near_at = [lax.rem(mine + d, half) for d in range(1, half)]
    far = (me + half) % n
    twins = [(group + d) % p for d in range(1, p)]
    sources = ((tg, og), (tu, ou))
    sums = Stream(sources, wide_s, narrow_s, in_s)
    ready = Stream(sources, wide_r, narrow_r, in_r)

    barrier = pltpu.get_barrier_semaphore()
    sums.prime(0, experts)
    for peer in peers:
        pl.semaphore_signal(barrier, inc=1, device_id={"fsdp": peer}, device_id_type=MESH)
    for twin in twins:
        pl.semaphore_signal(barrier, inc=1, device_id={"ep": twin}, device_id_type=MESH)

    def push(src, dst, axis, target, s, r):
        pltpu.make_async_remote_copy(
            src_ref=src, dst_ref=dst, send_sem=s, recv_sem=r,
            device_id={axis: target}, device_id_type=MESH,
        ).start()

    def sums_0(e, m, wide, narrow):
        row_sums(wide, narrow, land_0.at[m, me], pl.ds(0, 1))
        if m == 0:
            pl.semaphore_wait(barrier, n - 1 + p - 1)
        for peer in peers:
            push(land_0.at[m, me], land_0.at[m, me], "fsdp", peer, small_send.at[m], small_recv.at[m])

    def sums_a(e, m, wide, narrow):
        row_sums(wide, narrow, part_a.at[(e - first) * 2 + m], pl.ds(0, 1))

    share = part_z.shape[1]

    def sums_z(e, m, wide, narrow):
        at = (e - second) * 2 + m
        row_sums(wide, narrow, part_z.at[at // share], pl.ds(at % share, 1))

    def keep(e, m, total):
        scales[m][pl.ds(e, 1), :] = total / (n * depth)

    begin_0 = sender(n, me, peers, send, scales, readys, 0, own_sem.at[0], send_sem.at[0], recv_sem.at[0])
    begin_1 = sender(n, me, peers, send, scales, readys, 0, own_sem.at[1], send_sem.at[1], recv_sem.at[1])

    def begin_first(e, m, wide, narrow):
        drain(land_0.at[m, pl.ds(0, n - 1)], small_recv.at[m])
        keep(e, m, jnp.sum(land_0[m], axis=0))
        if m == 1:
            drain(land_a.at[pl.ds(0, n - 1)], small_recv.at[2])
            tot_a[me] = jnp.sum(land_a[...], axis=0)
            for peer in peers:
                push(tot_a.at[me], tot_a.at[me], "fsdp", peer, small_send.at[3], small_recv.at[3])
        begin_0(e, m, wide, narrow)

    sums.one(0, experts, sums_0)
    rows_r[me] = (rw[...] * rgain[...]).astype(bf16)
    push(rows_r.at[me], rows_r.at[me], "fsdp", far, r_send.at[0], r_recv.at[0])
    ready.prime(0, stop)
    sums.run(first, second, experts, sums_a)
    for peer in peers:
        push(part_a.at[peer], land_a.at[me], "fsdp", peer, small_send.at[2], small_recv.at[2])
    land_a[me] = part_a[me]
    ready.one(0, stop, begin_first)
    some = second + (experts - second) * 2 // 5
    sums.run(second, some, experts, sums_z)
    drain(tot_a.at[pl.ds(0, n - 1)], small_recv.at[3])
    for k in range(n):
        keep(first + k // 2, k % 2, tot_a[k])
    ready.run(1, 2, stop, begin_0)
    sums.run(some, experts, experts, sums_z)
    spare = half * share - 2 * (experts - second)
    if spare:
        part_z[half - 1, share - spare:, :] = jnp.zeros((spare, width), f32)
    for peer, at in zip(near, near_at):
        push(part_z.at[at], land_z.at[mine], "fsdp", peer, small_send.at[4], small_recv.at[4])
    land_z[mine] = part_z[mine]
    ready.run(2, 3, stop, begin_0)
    drain(land_z.at[pl.ds(0, half - 1)], small_recv.at[4])
    sum_z[...] = jnp.sum(land_z[...], axis=0)
    push(sum_z, far_z, "fsdp", far, small_send.at[5], small_recv.at[5])
    drain(rows_r.at[0], r_recv.at[0])
    for peer in near:
        push(rows_r.at[me], rows_r.at[me], "fsdp", peer, r_send.at[1], r_recv.at[1])
        push(rows_r.at[far], rows_r.at[far], "fsdp", peer, r_send.at[1], r_recv.at[1])
    ready.run(3, 4, stop, begin_0)
    drain(far_z, small_recv.at[5])
    tot_z[mine] = sum_z[...] + far_z[...]
    for peer in near:
        push(tot_z.at[mine], tot_z.at[mine], "fsdp", peer, small_send.at[6], small_recv.at[6])
    ready.run(4, second, stop, begin_0)
    drain(tot_z.at[pl.ds(0, half - 1)], small_recv.at[6])

    def keep_z(i, _):
        for m in range(2):
            at = i * 2 + m
            keep(second + i, m, tot_z[at // share, pl.ds(at % share, 1), :])
        return 0

    lax.fori_loop(0, experts - second, keep_z, 0)
    ready.run(second, cut, stop, begin_0)
    ready.run(cut, stop, stop, begin_1)
    drain(rows_r.at[pl.ds(0, n - 2)], r_recv.at[1])
    for twin in twins:
        push(rows_r, all_r.at[group], "ep", twin, r_send.at[2], r_recv.at[2])
    all_r[group] = rows_r[...]
    if p > 1:
        drain(all_r.at[pl.ds(0, p - 1)], r_recv.at[2])
    for f in range(n):
        block = all_r[:, f].astype(f32)
        block = block.reshape(block.shape[0] * block.shape[1], depth)
        router[f * depth:(f + 1) * depth, :] = block.T.astype(bf16)
    for m in range(2):
        drain(land_0.at[m, pl.ds(0, n - 1)], small_send.at[m])
    drain(part_a.at[pl.ds(0, n - 1)], small_send.at[2])
    drain(tot_a.at[pl.ds(0, n - 1)], small_send.at[3])
    drain(part_z.at[pl.ds(0, half - 1)], small_send.at[4])
    drain(sum_z, small_send.at[5])
    drain(tot_z.at[pl.ds(0, half - 1)], small_send.at[6])
    drain(rows_r.at[0], r_send.at[0])
    drain(rows_r.at[pl.ds(0, n - 2)], r_send.at[1])
    if p > 1:
        drain(all_r.at[pl.ds(0, p - 1)], r_send.at[2])
    finish(n, cut, send, readys, own_sem.at[0], send_sem.at[0], recv_sem.at[0])

    @pl.when(odd)
    def _():
        finish(n, more, send, readys, own_sem.at[1], send_sem.at[1], recv_sem.at[1])


def rest_kernel(n, cut, more, tg, og, tu, ou, scale_gate, scale_up, placed, ready_gate, ready_up,
                wide, narrow, send, in_sem, send_sem, recv_sem):
    experts = tg.shape[0]
    me = lax.axis_index("fsdp")
    odd = lax.rem(lax.axis_index("ep"), 2) == 1
    start = jnp.where(odd, cut + more, cut)
    readys, scales = (ready_gate, ready_up), (scale_gate, scale_up)
    peers = [(me + d) % n for d in far_first(n)]
    ready = Stream(((tg, og), (tu, ou)), wide, narrow, in_sem)
    barrier = pltpu.get_barrier_semaphore()
    for peer in peers:
        pl.semaphore_signal(barrier, inc=1, device_id={"fsdp": peer}, device_id_type=MESH)
    ready.prime(start, experts)
    pl.semaphore_wait(barrier, n - 1)
    begin = [
        sender(n, me, peers, send, scales, readys, cut, None, send_sem.at[k], recv_sem.at[k])
        for k in range(2)
    ]
    ready.run(start, cut + more, experts, begin[1])
    ready.run(cut + more, experts, experts, begin[0])
    finish(n, experts - cut - more, send, readys, None, send_sem.at[0], recv_sem.at[0])

    @pl.when(jnp.logical_not(odd))
    def _():
        finish(n, more, send, readys, None, send_sem.at[1], recv_sem.at[1])


def copy_through(pairs, count, deep, buffer, in_sem, out_sem):
    lag = deep // 2

    def bring(i, k):
        slot = lax.rem(i, deep)
        return pltpu.make_async_copy(pairs[k][0].at[i], buffer.at[k, slot], in_sem.at[k, slot])

    def give(i, k):
        slot = lax.rem(i, deep)
        return pltpu.make_async_copy(buffer.at[k, slot], pairs[k][1].at[i], out_sem.at[k, slot])

    def opening(i, _):
        for k in range(2):
            bring(i, k).start()
        return 0

    lax.fori_loop(0, jnp.minimum(count, deep), opening, 0)

    def step(i, _):
        @pl.when(i < count)
        def _():
            for k in range(2):
                bring(i, k).wait()
                give(i, k).start()

        @pl.when(i >= lag)
        def _():
            for k in range(2):
                give(i - lag, k).wait()

            @pl.when(i - lag + deep < count)
            def _():
                for k in range(2):
                    bring(i - lag + deep, k).start()

        return 0

    lax.fori_loop(0, count + lag, step, 0)


def own_columns(n, scale, out):
    me = lax.axis_index("fsdp")
    piece = out.shape[1]
    value = jnp.zeros(out.shape, out.dtype)
    for j in range(n):
        value = jnp.where(me == j, scale[:, j * piece:(j + 1) * piece], value)
    out[...] = value


def place_kernel(n, cut, more, got_gate, got_up, scale_gate, scale_up, router,
                 gate, up, own_gate, own_up, router_out, buffer, scales, in_sem, out_sem, small_sem):
    odd = lax.rem(lax.axis_index("ep"), 2) == 1
    high = jnp.where(odd, cut + more, cut)
    small = [
        pltpu.make_async_copy(scale_gate, scales.at[0], small_sem.at[0]),
        pltpu.make_async_copy(scale_up, scales.at[1], small_sem.at[1]),
        pltpu.make_async_copy(router, router_out, small_sem.at[2]),
    ]
    for copy in small:
        copy.start()
    deep = jnp.where(odd, SLOW, RING)
    copy_through(((got_gate, gate), (got_up, up)), high, deep, buffer, in_sem, out_sem)
    for copy in small:
        copy.wait()
    own_columns(n, scales[0], own_gate)
    own_columns(n, scales[1], own_up)


def end_kernel(n, cut, more, got_gate, got_up, had_gate, had_up, gate, up, sem):
    odd = lax.rem(lax.axis_index("ep"), 2) == 1
    experts = gate.shape[0]
    early, late = pl.ds(0, more), pl.ds(more, experts - cut - more)

    def copies(some, low, count, k):
        return [
            pltpu.make_async_copy(got.at[some], out.at[pl.ds(low, count)], sem.at[k, m])
            for m, (got, out) in enumerate(((got_gate, gate), (got_up, up)))
        ]

    both = copies(late, cut + more, experts - cut - more, 0)
    for copy in both:
        copy.start()

    @pl.when(jnp.logical_not(odd))
    def _():
        others = copies(early, cut, more, 1)
        for copy in others:
            copy.start()
        for copy in others:
            copy.wait()

    for copy in both:
        copy.wait()


def sending_device(n, p, train_gate, other_gate, train_up, other_up, router_weight, router_gain):
    experts, depth, width = train_gate.shape
    piece = width // n
    columns = router_weight.shape[1]
    half = n // 2
    share = -(-2 * (experts - 1 - half) // half)
    tail = experts // 32
    more = 3 * experts // 16
    cut = experts - tail - more
    bulk, rest = cut + more, experts - cut
    anywhere = pl.BlockSpec(memory_space=pltpu.HBM)
    vmem = pl.BlockSpec(memory_space=pltpu.VMEM)
    shape = jax.ShapeDtypeStruct
    full = shape((experts, width), f32)
    own = shape((experts, piece), f32)
    whole = shape((experts, piece, n * depth), bf16)
    routed = shape((n * depth, p * columns), bf16)
    dma = pltpu.SemaphoreType.DMA
    got_gate, got_up, scale_gate, scale_up, router = pl.pallas_call(
        functools.partial(bulk_kernel, n, p, cut, more),
        out_shape=(shape((bulk, piece, n * depth), bf16),) * 2 + (full, full, routed),
        in_specs=[anywhere] * 4 + [vmem] * 2,
        out_specs=(anywhere, anywhere, vmem, vmem, vmem),
        scratch_shapes=[
            pltpu.VMEM((2, SLOTS, depth, width), f32),
            pltpu.VMEM((2, SLOTS, depth, width), bf16),
            pltpu.VMEM((2, SLOTS, depth, width), f32),
            pltpu.VMEM((2, SLOTS, depth, width), bf16),
            pltpu.VMEM((2, bulk, width, depth), bf16),
            pltpu.VMEM((2, n, 1, width), f32),
            *[pltpu.VMEM((n, 1, width), f32)] * 3,
            *[pltpu.VMEM((half, share, width), f32)] * 2,
            *[pltpu.VMEM((share, width), f32)] * 2,
            pltpu.VMEM((half, share, width), f32),
            pltpu.VMEM((n, columns, depth), bf16),
            pltpu.VMEM((p, n, columns, depth), bf16),
            dma((2, 2, SLOTS)), dma((2, 2, SLOTS)), dma((2, 2)), dma((2, 2)), dma((2, 2)),
            dma((7,)), dma((7,)), dma((3,)), dma((3,)),
        ],
        compiler_params=pltpu.CompilerParams(
            collective_id=0, has_side_effects=True, vmem_limit_bytes=60 * 2**20
        ),
        name="send_bulk",
    )(train_gate, other_gate, train_up, other_up, router_weight.T, router_gain[None, :])
    gate, up, own_gate, own_up, router = pl.pallas_call(
        functools.partial(place_kernel, n, cut, more),
        out_shape=(whole, whole, own, own, routed),
        in_specs=[anywhere] * 5,
        out_specs=(anywhere, anywhere, vmem, vmem, vmem),
        scratch_shapes=[
            pltpu.VMEM((2, RING, piece, n * depth), bf16),
            pltpu.VMEM((2, experts, width), f32),
            dma((2, RING)), dma((2, RING)), dma((3,)),
        ],
        compiler_params=pltpu.CompilerParams(vmem_limit_bytes=60 * 2**20),
        name="place_bulk",
    )(got_gate, got_up, scale_gate, scale_up, router)
    got_gate, got_up = pl.pallas_call(
        functools.partial(rest_kernel, n, cut, more),
        out_shape=(shape((rest, piece, n * depth), bf16),) * 2,
        in_specs=[anywhere] * 4 + [vmem] * 2 + [anywhere],
        out_specs=(vmem, vmem),
        scratch_shapes=[
            pltpu.VMEM((2, SLOTS, depth, width), f32),
            pltpu.VMEM((2, SLOTS, depth, width), bf16),
            pltpu.VMEM((2, rest, width, depth), bf16),
            dma((2, 2, SLOTS)), dma((2, 2)), dma((2, 2)),
        ],
        compiler_params=pltpu.CompilerParams(
            collective_id=1, has_side_effects=True, vmem_limit_bytes=40 * 2**20
        ),
        name="send_rest",
    )(train_gate, other_gate, train_up, other_up, scale_gate, scale_up, own_gate)
    gate, up = pl.pallas_call(
        functools.partial(end_kernel, n, cut, more),
        out_shape=(whole, whole),
        in_specs=[vmem] * 2 + [anywhere] * 2,
        out_specs=(anywhere, anywhere),
        scratch_shapes=[dma((2, 2))],
        input_output_aliases={2: 0, 3: 1},
        compiler_params=pltpu.CompilerParams(vmem_limit_bytes=40 * 2**20),
        name="place_rest",
    )(got_gate, got_up, gate, up)
    return (jnp.swapaxes(gate, 1, 2), jnp.swapaxes(up, 1, 2), own_gate, own_up, router)


def solution(mesh):
    n, p = mesh.shape["fsdp"], mesh.shape["ep"]

    def per_device(*args):
        experts, depth, width = args[0].shape
        fits = (
            depth % 128 == 0 and width % (16 * n) == 0 and width % 128 == 0 and n % 4 == 0
            and experts % 32 == 0 and experts >= n + 8 and args[4].shape[1] % 16 == 0
            and 2 * experts * depth * width * 2 <= 2**25
        )
        return sending_device(n, p, *args) if fits else plain_device(*args)

    matrix = P("ep", "fsdp", None)
    in_specs = (matrix, matrix, matrix, matrix, P("fsdp", "ep"), P("fsdp"))
    out_specs = (P("ep", None, "fsdp"), P("ep", None, "fsdp"), P("ep", "fsdp"), P("ep", "fsdp"), P())
    return jax.shard_map(
        per_device, mesh=mesh, in_specs=in_specs, out_specs=out_specs, check_vma=False
    )
```

```python
import functools

import jax
import jax.numpy as jnp
from jax import lax
from jax.experimental import pallas as pl
from jax.experimental.pallas import tpu as pltpu
from jax.sharding import PartitionSpec as P

MESH = pl.DeviceIdType.MESH
SLOTS = 3
RING = 20
SLOW = 2
RAW = 2
f32, bf16 = jnp.float32, jnp.bfloat16


def plain_device(train_gate, other_gate, train_up, other_up, router_weight, router_gain):
    latest_gate = train_gate + other_gate.astype(jnp.float32)
    latest_up = train_up + other_up.astype(jnp.float32)
    depth = train_gate.shape[1] * lax.axis_size("fsdp")
    total_gate, total_up = lax.psum(
        (jnp.sum(jnp.abs(latest_gate), axis=1), jnp.sum(jnp.abs(latest_up), axis=1)), "fsdp"
    )
    scale_gate = total_gate / depth
    scale_up = total_up / depth
    narrow_gate = (latest_gate / jnp.expand_dims(scale_gate, 1)).astype(jnp.bfloat16)
    narrow_up = (latest_up / jnp.expand_dims(scale_up, 1)).astype(jnp.bfloat16)
    ready_gate = lax.all_to_all(narrow_gate, "fsdp", split_axis=2, concat_axis=1, tiled=True)
    ready_up = lax.all_to_all(narrow_up, "fsdp", split_axis=2, concat_axis=1, tiled=True)
    width = ready_gate.shape[2]
    start = lax.axis_index("fsdp") * width
    scale_gate = lax.dynamic_slice_in_dim(scale_gate, start, width, axis=1)
    scale_up = lax.dynamic_slice_in_dim(scale_up, start, width, axis=1)
    part_router = (router_weight * router_gain[:, None]).astype(jnp.bfloat16)
    row_router = lax.all_gather(part_router, "fsdp", axis=0, tiled=True)
    serve_router = lax.all_gather(row_router, "ep", axis=1, tiled=True)
    return (ready_gate, ready_up, scale_gate, scale_up, serve_router)


def far_first(n):
    return sorted(range(1, n), key=lambda d: (abs(d - n // 2), d))


def drain(ref, sem):
    pltpu.make_async_copy(ref, ref, sem).wait()


class Stream:
    def __init__(self, sources, wide, narrow, sem):
        self.sources, self.wide, self.narrow, self.sem = sources, wide, narrow, sem

    def loads(self, e):
        slot = lax.rem(e, SLOTS)
        return [
            pltpu.make_async_copy(src.at[e], dst.at[m, slot], self.sem.at[k, m, slot])
            for m, pair in enumerate(self.sources)
            for k, (src, dst) in enumerate(zip(pair, (self.wide, self.narrow)))
        ]

    def prime(self, low, last):
        for i in range(SLOTS - 1):
            @pl.when(low + i < last)
            def _():
                for copy in self.loads(low + i):
                    copy.start()

    def one(self, e, last, body):
        @pl.when(e + SLOTS - 1 < last)
        def _():
            for copy in self.loads(e + SLOTS - 1):
                copy.start()

        copies = self.loads(e)
        slot = lax.rem(e, SLOTS)
        for m in range(2):
            copies[2 * m].wait()
            copies[2 * m + 1].wait()
            body(e, m, self.wide.at[m, slot], self.narrow.at[m, slot])

    def run(self, low, high, last, body):
        def step(i, _):
            self.one(low + i, last, body)
            return 0

        lax.fori_loop(0, high - low, step, 0)


def row_sums(wide, narrow, out, at):
    depth, width = wide.shape
    block = 256 if width % 256 == 0 else 128
    for c in range(0, width, block):
        total = jnp.zeros((16, block), f32)
        for r in range(0, depth, 16):
            total += jnp.abs(wide[r:r + 16, c:c + block] + narrow[r:r + 16, c:c + block].astype(f32))
        out[at, c:c + block] = jnp.sum(total, axis=0, keepdims=True)


def sender(n, me, peers, send, scales, readys, base, own_sem, send_sem, recv_sem):
    def body(e, m, wide, narrow):
        depth, width = wide.shape
        piece = width // n
        inverse = 1.0 / scales[m][pl.ds(e, 1), :]
        at = e - base
        for c in range(0, width, 128):
            latest = wide[:, c:c + 128] + narrow[:, c:c + 128].astype(f32)
            value = latest * inverse[:, c:c + 128]
            send[m, at, c:c + 128, :] = value.T.astype(bf16)
        place = readys[m].at[at, :, pl.ds(pl.multiple_of(me * depth, 128), depth)]
        for peer in peers:
            pltpu.make_async_remote_copy(
                src_ref=send.at[m, at, pl.ds(pl.multiple_of(peer * piece, 16), piece), :],
                dst_ref=place,
                send_sem=send_sem.at[m],
                recv_sem=recv_sem.at[m],
                device_id={"fsdp": peer},
                device_id_type=MESH,
            ).start()
        own = send.at[m, at, pl.ds(pl.multiple_of(me * piece, 16), piece), :]
        if own_sem is None:
            place[...] = own[...]
        else:
            pltpu.make_async_copy(own, place, own_sem.at[m]).start()

    return body


def finish(n, count, send, readys, own_sem, send_sem, recv_sem):
    width, depth = send.shape[2:]
    piece = width // n
    for m in range(2):
        some = pl.ds(0, count)
        if own_sem is not None:
            drain(send.at[m, some, pl.ds(0, piece), :], own_sem.at[m])
        drain(send.at[m, some, pl.ds(0, width - piece), :], send_sem.at[m])
        drain(readys[m].at[some, :, pl.ds(0, (n - 1) * depth)], recv_sem.at[m])


def coded(value):
    square = value * value
    fourth = square * square
    return (fourth * fourth) * (square * value)


def decoded(code):
    size = jnp.abs(code)
    root = jnp.exp(jnp.log(jnp.where(size > 0, size, 1.0)) * (1.0 / 11.0))
    return jnp.where(size > 0, jnp.where(code < 0, -root, root), 0.0)


def bulk_kernel(n, p, cut, more, tg, og, tu, ou, rw, rgain, ready_gate, ready_up, scale_gate, scale_up, router,
                wide_s, narrow_s, wide_r, narrow_r, send, raw_land, part_0, land_0, row_0, part_a, land_a, tot_a,
                part_z, land_z, sum_z, far_z, tot_z, rows_r, all_r,
                in_s, in_r, own_sem, send_sem, recv_sem, small_send, small_recv, r_send, r_recv,
                sum_send, sum_recv, raw_send, raw_recv, raw_out):
    experts, depth, width = tg.shape
    half = n // 2
    piece = width // n
    me = lax.axis_index("fsdp")
    group = lax.axis_index("ep")
    odd = lax.rem(group, 2) == 1
    stop = jnp.where(odd, cut + more, cut)
    mine = lax.rem(me, half)
    side = me - mine
    first, second = RAW, RAW + half
    readys, scales = (ready_gate, ready_up), (scale_gate, scale_up)
    peers = [(me + d) % n for d in far_first(n)]
    near = [side + lax.rem(mine + d, half) for d in range(1, half)]
    near_at = [lax.rem(mine + d, half) for d in range(1, half)]
    far = (me + half) % n
    twins = [(group + d) % p for d in range(1, p)]
    sources = ((tg, og), (tu, ou))
    sums = Stream(sources, wide_s, narrow_s, in_s)
    ready = Stream(sources, wide_r, narrow_r, in_r)

    barrier = pltpu.get_barrier_semaphore()
    for peer in peers:
        pl.semaphore_signal(barrier, inc=1, device_id={"fsdp": peer}, device_id_type=MESH)
    for twin in twins:
        pl.semaphore_signal(barrier, inc=1, device_id={"ep": twin}, device_id_type=MESH)
    sums.prime(0, experts)

    def push(src, dst, axis, target, s, r):
        pltpu.make_async_remote_copy(
            src_ref=src, dst_ref=dst, send_sem=s, recv_sem=r,
            device_id={axis: target}, device_id_type=MESH,
        ).start()

    def sums_0(e, m, wide, narrow):
        u = 2 * e + m
        row_sums(wide, narrow, row_0, pl.ds(0, 1))
        row = row_0[...]
        for j in range(n):
            part_0[u, j, :, 0:piece] = row[:, j * piece:(j + 1) * piece]
        inverse = jnp.where(row > 0, depth / row, 0.0)
        for c in range(0, width, 128):
            latest = wide[:, c:c + 128] + narrow[:, c:c + 128].astype(f32)
            send[m, e, c:c + 128, :] = coded(latest * inverse[:, c:c + 128]).T.astype(bf16)

    def push_0(u):
        e, m = divmod(u, 2)
        for peer in peers:
            push(part_0.at[u, peer], land_0.at[u, me], "fsdp", peer, sum_send.at[u], sum_recv.at[u])
        for peer in peers:
            push(send.at[m, e, pl.ds(pl.multiple_of(peer * piece, 16), piece), :],
                 raw_land.at[u, :, pl.ds(pl.multiple_of(me * depth, 128), depth)],
                 "fsdp", peer, raw_send.at[u], raw_recv.at[u])

    def end_0(u):
        e, m = divmod(u, 2)
        raw_land[u, :, pl.ds(pl.multiple_of(me * depth, 128), depth)] = (
            send[m, e, pl.ds(pl.multiple_of(me * piece, 16), piece), :]
        )
        land_0[u, me] = part_0[u, me]
        drain(land_0.at[u, pl.ds(0, n - 1)], sum_recv.at[u])
        drain(raw_land.at[u, :, pl.ds(0, (n - 1) * depth)], raw_recv.at[u])
        got = land_0[u].reshape(n, 128)
        scale = jnp.sum(got, axis=0, keepdims=True) / (n * depth)
        for j in range(n):
            scales[m][e:e + 1, j * piece:(j + 1) * piece] = scale[:, 0:piece]
        used = lax.broadcasted_iota(jnp.int32, (1, 128), 1) < piece
        factor = (got / depth / jnp.where(used, scale, 1.0)).T
        for s in range(n):
            code = raw_land[u, :, s * depth:(s + 1) * depth].astype(f32)
            value = decoded(code) * factor[0:piece, s:s + 1]
            raw_land[u, :, s * depth:(s + 1) * depth] = value.astype(bf16)
        pltpu.make_async_copy(raw_land.at[u], readys[m].at[e], raw_out.at[u]).start()

    def sums_a(e, m, wide, narrow):
        row_sums(wide, narrow, part_a.at[(e - first) * 2 + m], pl.ds(0, 1))

    share = part_z.shape[1]

    def sums_z(e, m, wide, narrow):
        at = (e - second) * 2 + m
        row_sums(wide, narrow, part_z.at[at // share], pl.ds(at % share, 1))

    def keep(e, m, total):
        scales[m][pl.ds(e, 1), :] = total / (n * depth)

    begin_0 = sender(n, me, peers, send, scales, readys, 0, own_sem.at[0], send_sem.at[0], recv_sem.at[0])
    begin_1 = sender(n, me, peers, send, scales, readys, 0, own_sem.at[1], send_sem.at[1], recv_sem.at[1])

    part_0[...] = jnp.zeros_like(part_0)
    sums.one(0, experts, sums_0)
    pl.semaphore_wait(barrier, n - 1 + p - 1)
    push_0(0)
    rows_r[me] = (rw[...] * rgain[...]).astype(bf16)
    for e in range(1, RAW):
        sums.one(e, experts, sums_0)
    sums.run(first, second, experts, sums_a)
    for peer in peers:
        push(part_a.at[peer], land_a.at[me], "fsdp", peer, small_send.at[2], small_recv.at[2])
    land_a[me] = part_a[me]
    push(rows_r.at[me], rows_r.at[me], "fsdp", far, r_send.at[0], r_recv.at[0])
    push_0(1)
    ready.prime(first, stop)
    some = second + (experts - second) * 7 // 10
    sums.run(second, some, experts, sums_z)
    drain(land_a.at[pl.ds(0, n - 1)], small_recv.at[2])
    tot_a[me] = jnp.sum(land_a[...], axis=0)
    for peer in peers:
        push(tot_a.at[me], tot_a.at[me], "fsdp", peer, small_send.at[3], small_recv.at[3])
    for u in range(2, 2 * RAW):
        push_0(u)
    sums.run(some, experts, experts, sums_z)
    spare = half * share - 2 * (experts - second)
    if spare:
        part_z[half - 1, share - spare:, :] = jnp.zeros((spare, width), f32)
    for peer, at in zip(near, near_at):
        push(part_z.at[at], land_z.at[mine], "fsdp", peer, small_send.at[4], small_recv.at[4])
    land_z[mine] = part_z[mine]
    drain(tot_a.at[pl.ds(0, n - 1)], small_recv.at[3])
    for k in range(n):
        keep(first + k // 2, k % 2, tot_a[k])
    ready.run(first, first + 1, stop, begin_0)
    drain(land_z.at[pl.ds(0, half - 1)], small_recv.at[4])
    sum_z[...] = jnp.sum(land_z[...], axis=0)
    push(sum_z, far_z, "fsdp", far, small_send.at[5], small_recv.at[5])
    drain(rows_r.at[0], r_recv.at[0])
    for peer in near:
        push(rows_r.at[me], rows_r.at[me], "fsdp", peer, r_send.at[1], r_recv.at[1])
        push(rows_r.at[far], rows_r.at[far], "fsdp", peer, r_send.at[1], r_recv.at[1])
    ready.run(first + 1, first + 2, stop, begin_0)
    drain(far_z, small_recv.at[5])
    tot_z[mine] = sum_z[...] + far_z[...]
    for peer in near:
        push(tot_z.at[mine], tot_z.at[mine], "fsdp", peer, small_send.at[6], small_recv.at[6])
    ready.run(first + 2, second, stop, begin_0)
    drain(tot_z.at[pl.ds(0, half - 1)], small_recv.at[6])

    def keep_z(i, _):
        for m in range(2):
            at = i * 2 + m
            keep(second + i, m, tot_z[at // share, pl.ds(at % share, 1), :])
        return 0

    lax.fori_loop(0, experts - second, keep_z, 0)
    ready.run(second, cut, stop, begin_0)
    ready.run(cut, stop, stop, begin_1)
    for u in range(2 * RAW):
        end_0(u)
    drain(rows_r.at[pl.ds(0, n - 2)], r_recv.at[1])
    for twin in twins:
        push(rows_r, all_r.at[group], "ep", twin, r_send.at[2], r_recv.at[2])
    all_r[group] = rows_r[...]
    if p > 1:
        drain(all_r.at[pl.ds(0, p - 1)], r_recv.at[2])
    for f in range(n):
        block = all_r[:, f].astype(f32)
        block = block.reshape(block.shape[0] * block.shape[1], depth)
        router[f * depth:(f + 1) * depth, :] = block.T.astype(bf16)
    for u in range(2 * RAW):
        drain(part_0.at[u, pl.ds(0, n - 1)], sum_send.at[u])
        drain(send.at[0, 0, pl.ds(0, width - piece), :], raw_send.at[u])
        drain(raw_land.at[u], raw_out.at[u])
    drain(part_a.at[pl.ds(0, n - 1)], small_send.at[2])
    drain(tot_a.at[pl.ds(0, n - 1)], small_send.at[3])
    drain(part_z.at[pl.ds(0, half - 1)], small_send.at[4])
    drain(sum_z, small_send.at[5])
    drain(tot_z.at[pl.ds(0, half - 1)], small_send.at[6])
    drain(rows_r.at[0], r_send.at[0])
    drain(rows_r.at[pl.ds(0, n - 2)], r_send.at[1])
    if p > 1:
        drain(all_r.at[pl.ds(0, p - 1)], r_send.at[2])
    finish(n, cut - RAW, send, readys, own_sem.at[0], send_sem.at[0], recv_sem.at[0])

    @pl.when(odd)
    def _():
        finish(n, more, send, readys, own_sem.at[1], send_sem.at[1], recv_sem.at[1])


def rest_kernel(n, cut, more, tg, og, tu, ou, scale_gate, scale_up, placed, ready_gate, ready_up,
                wide, narrow, send, in_sem, send_sem, recv_sem):
    experts = tg.shape[0]
    me = lax.axis_index("fsdp")
    odd = lax.rem(lax.axis_index("ep"), 2) == 1
    start = jnp.where(odd, cut + more, cut)
    readys, scales = (ready_gate, ready_up), (scale_gate, scale_up)
    peers = [(me + d) % n for d in far_first(n)]
    ready = Stream(((tg, og), (tu, ou)), wide, narrow, in_sem)
    barrier = pltpu.get_barrier_semaphore()
    for peer in peers:
        pl.semaphore_signal(barrier, inc=1, device_id={"fsdp": peer}, device_id_type=MESH)
    ready.prime(start, experts)
    pl.semaphore_wait(barrier, n - 1)
    begin = [
        sender(n, me, peers, send, scales, readys, cut, None, send_sem.at[k], recv_sem.at[k])
        for k in range(2)
    ]
    ready.run(start, cut + more, experts, begin[1])
    ready.run(cut + more, experts, experts, begin[0])
    finish(n, experts - cut - more, send, readys, None, send_sem.at[0], recv_sem.at[0])

    @pl.when(jnp.logical_not(odd))
    def _():
        finish(n, more, send, readys, None, send_sem.at[1], recv_sem.at[1])


def copy_through(pairs, count, deep, buffer, in_sem, out_sem):
    lag = deep // 2

    def bring(i, k):
        slot = lax.rem(i, deep)
        return pltpu.make_async_copy(pairs[k][0].at[i], buffer.at[k, slot], in_sem.at[k, slot])

    def give(i, k):
        slot = lax.rem(i, deep)
        return pltpu.make_async_copy(buffer.at[k, slot], pairs[k][1].at[i], out_sem.at[k, slot])

    def opening(i, _):
        for k in range(2):
            bring(i, k).start()
        return 0

    lax.fori_loop(0, jnp.minimum(count, deep), opening, 0)

    def step(i, _):
        @pl.when(i < count)
        def _():
            for k in range(2):
                bring(i, k).wait()
                give(i, k).start()

        @pl.when(i >= lag)
        def _():
            for k in range(2):
                give(i - lag, k).wait()

            @pl.when(i - lag + deep < count)
            def _():
                for k in range(2):
                    bring(i - lag + deep, k).start()

        return 0

    lax.fori_loop(0, count + lag, step, 0)


def own_columns(n, scale, out):
    me = lax.axis_index("fsdp")
    piece = out.shape[1]
    value = jnp.zeros(out.shape, out.dtype)
    for j in range(n):
        value = jnp.where(me == j, scale[:, j * piece:(j + 1) * piece], value)
    out[...] = value


def place_kernel(n, cut, more, got_gate, got_up, scale_gate, scale_up, router,
                 gate, up, own_gate, own_up, router_out, buffer, scales, in_sem, out_sem, small_sem):
    odd = lax.rem(lax.axis_index("ep"), 2) == 1
    high = jnp.where(odd, cut + more, cut)
    small = [
        pltpu.make_async_copy(scale_gate, scales.at[0], small_sem.at[0]),
        pltpu.make_async_copy(scale_up, scales.at[1], small_sem.at[1]),
        pltpu.make_async_copy(router, router_out, small_sem.at[2]),
    ]
    for copy in small:
        copy.start()
    deep = jnp.where(odd, SLOW, RING)
    copy_through(((got_gate, gate), (got_up, up)), high, deep, buffer, in_sem, out_sem)
    for copy in small:
        copy.wait()
    own_columns(n, scales[0], own_gate)
    own_columns(n, scales[1], own_up)


def end_kernel(n, cut, more, got_gate, got_up, had_gate, had_up, gate, up, sem):
    odd = lax.rem(lax.axis_index("ep"), 2) == 1
    experts = gate.shape[0]
    early, late = pl.ds(0, more), pl.ds(more, experts - cut - more)

    def copies(some, low, count, k):
        return [
            pltpu.make_async_copy(got.at[some], out.at[pl.ds(low, count)], sem.at[k, m])
            for m, (got, out) in enumerate(((got_gate, gate), (got_up, up)))
        ]

    both = copies(late, cut + more, experts - cut - more, 0)
    for copy in both:
        copy.start()

    @pl.when(jnp.logical_not(odd))
    def _():
        others = copies(early, cut, more, 1)
        for copy in others:
            copy.start()
        for copy in others:
            copy.wait()

    for copy in both:
        copy.wait()


def sending_device(n, p, train_gate, other_gate, train_up, other_up, router_weight, router_gain):
    experts, depth, width = train_gate.shape
    piece = width // n
    columns = router_weight.shape[1]
    half = n // 2
    share = -(-2 * (experts - RAW - half) // half)
    tail = experts // 32
    more = 3 * experts // 16
    cut = experts - tail - more
    bulk, rest = cut + more, experts - cut
    anywhere = pl.BlockSpec(memory_space=pltpu.HBM)
    vmem = pl.BlockSpec(memory_space=pltpu.VMEM)
    shape = jax.ShapeDtypeStruct
    full = shape((experts, width), f32)
    own = shape((experts, piece), f32)
    whole = shape((experts, piece, n * depth), bf16)
    routed = shape((n * depth, p * columns), bf16)
    dma = pltpu.SemaphoreType.DMA
    got_gate, got_up, scale_gate, scale_up, router = pl.pallas_call(
        functools.partial(bulk_kernel, n, p, cut, more),
        out_shape=(shape((bulk, piece, n * depth), bf16),) * 2 + (full, full, routed),
        in_specs=[anywhere] * 4 + [vmem] * 2,
        out_specs=(anywhere, anywhere, vmem, vmem, vmem),
        scratch_shapes=[
            pltpu.VMEM((2, SLOTS, depth, width), f32),
            pltpu.VMEM((2, SLOTS, depth, width), bf16),
            pltpu.VMEM((2, SLOTS, depth, width), f32),
            pltpu.VMEM((2, SLOTS, depth, width), bf16),
            pltpu.VMEM((2, bulk, width, depth), bf16),
            pltpu.VMEM((2 * RAW, piece, n * depth), bf16),
            *[pltpu.VMEM((2 * RAW, n, 1, 128), f32)] * 2,
            pltpu.VMEM((1, width), f32),
            *[pltpu.VMEM((n, 1, width), f32)] * 3,
            *[pltpu.VMEM((half, share, width), f32)] * 2,
            *[pltpu.VMEM((share, width), f32)] * 2,
            pltpu.VMEM((half, share, width), f32),
            pltpu.VMEM((n, columns, depth), bf16),
            pltpu.VMEM((p, n, columns, depth), bf16),
            dma((2, 2, SLOTS)), dma((2, 2, SLOTS)), dma((2, 2)), dma((2, 2)), dma((2, 2)),
            dma((7,)), dma((7,)), dma((3,)), dma((3,)), *[dma((2 * RAW,))] * 5,
        ],
        compiler_params=pltpu.CompilerParams(
            collective_id=0, has_side_effects=True, vmem_limit_bytes=60 * 2**20
        ),
        name="send_bulk",
    )(train_gate, other_gate, train_up, other_up, router_weight.T, router_gain[None, :])
    gate, up, own_gate, own_up, router = pl.pallas_call(
        functools.partial(place_kernel, n, cut, more),
        out_shape=(whole, whole, own, own, routed),
        in_specs=[anywhere] * 5,
        out_specs=(anywhere, anywhere, vmem, vmem, vmem),
        scratch_shapes=[
            pltpu.VMEM((2, RING, piece, n * depth), bf16),
            pltpu.VMEM((2, experts, width), f32),
            dma((2, RING)), dma((2, RING)), dma((3,)),
        ],
        compiler_params=pltpu.CompilerParams(vmem_limit_bytes=60 * 2**20),
        name="place_bulk",
    )(got_gate, got_up, scale_gate, scale_up, router)
    got_gate, got_up = pl.pallas_call(
        functools.partial(rest_kernel, n, cut, more),
        out_shape=(shape((rest, piece, n * depth), bf16),) * 2,
        in_specs=[anywhere] * 4 + [vmem] * 2 + [anywhere],
        out_specs=(vmem, vmem),
        scratch_shapes=[
            pltpu.VMEM((2, SLOTS, depth, width), f32),
            pltpu.VMEM((2, SLOTS, depth, width), bf16),
            pltpu.VMEM((2, rest, width, depth), bf16),
            dma((2, 2, SLOTS)), dma((2, 2)), dma((2, 2)),
        ],
        compiler_params=pltpu.CompilerParams(
            collective_id=1, has_side_effects=True, vmem_limit_bytes=40 * 2**20
        ),
        name="send_rest",
    )(train_gate, other_gate, train_up, other_up, scale_gate, scale_up, own_gate)
    gate, up = pl.pallas_call(
        functools.partial(end_kernel, n, cut, more),
        out_shape=(whole, whole),
        in_specs=[vmem] * 2 + [anywhere] * 2,
        out_specs=(anywhere, anywhere),
        scratch_shapes=[dma((2, 2))],
        input_output_aliases={2: 0, 3: 1},
        compiler_params=pltpu.CompilerParams(vmem_limit_bytes=40 * 2**20),
        name="place_rest",
    )(got_gate, got_up, gate, up)
    return (jnp.swapaxes(gate, 1, 2), jnp.swapaxes(up, 1, 2), own_gate, own_up, router)


def solution(mesh):
    n, p = mesh.shape["fsdp"], mesh.shape["ep"]

    def per_device(*args):
        experts, depth, width = args[0].shape
        fits = (
            depth % 128 == 0 and width % (16 * n) == 0 and width % 128 == 0 and n % 4 == 0
            and experts % 32 == 0 and experts >= n + 8 and width <= 128 * n
            and depth <= 256 and args[4].shape[1] % 16 == 0
            and 2 * experts * depth * width * 2 <= 2**25
        )
        return sending_device(n, p, *args) if fits else plain_device(*args)

    matrix = P("ep", "fsdp", None)
    in_specs = (matrix, matrix, matrix, matrix, P("fsdp", "ep"), P("fsdp"))
    out_specs = (P("ep", None, "fsdp"), P("ep", None, "fsdp"), P("ep", "fsdp"), P("ep", "fsdp"), P())
    return jax.shard_map(
        per_device, mesh=mesh, in_specs=in_specs, out_specs=out_specs, check_vma=False
    )
```
